256 devices in a mesh: mp: 64 (over y, z, core), dp: 4 (over x).
Axes of the slice: x: 4, y: 4, z: 8, core: 2. Of those that a mesh axis runs over, the one named last changes fastest.
Arguments:
- features: bfloat16 [256, 4, 4, 512], P(('dp', 'mp')), may hold values from 0 to 2
- labels: int32 [256], P('dp'), may hold values from 0 to 9
- subset_ids: int32 [64], P('mp'), may hold values from 0 to 255
- conv1_weight: bfloat16 [64, 9, 512, 512], P('mp'), may hold values from -0.09375 to 0.09375
- conv2_weight: bfloat16 [64, 9, 512, 512], P('mp'), may hold values from -0.09375 to 0.09375
- head_weight: float32 [64, 512, 10], P('mp'), may hold values from -0.25 to 0.25
Outputs:
- datamodel: float32 [256, 256], P(('dp', 'mp'))
- margin_mean: float32 [256], P(('dp', 'mp'))
- margin_norm: float32 [256], P(('dp', 'mp'))
The draws below stay inside these ranges and needn't reach their ends.
All inputs are finite; a program needn't handle non-finite values.
Results may differ from the reference program's by a relative error of at most 0.00077.
Values may be sent and summed in bfloat16 or wider, within the bound.
A program may use at most 128 MiB of HBM per device.

```python
import jax
import jax.numpy as jnp
from jax import lax

C = 512
CLASSES = 10
SIDE = 4
SUBSETS = 256
TARGETS = 256
MODELS = 64


def with_ends(entries, own_key, low, high):
    dims = entries.shape
    spot = [jax.random.randint(jax.random.fold_in(own_key, axis), (), 0, dims[axis]) for axis in range(len(dims))]
    entries = entries.at[tuple(spot)].set(low)
    longest = dims.index(max(dims))
    spot[longest] = (spot[longest] + 1) % dims[longest]
    return entries.at[tuple(spot)].set(high)


def block_levels(key, shape, cuts, smallest, top_value):
    level = 1.0
    for dim, shards_of in cuts:
        draws = jax.random.uniform(jax.random.fold_in(jax.random.fold_in(key, 6), dim), (shards_of,), jnp.float32, smallest / len(cuts), top_value / len(cuts))
        level = level * jnp.repeat(jnp.exp(draws), shape[dim] // shards_of).reshape((-1,) + (1,) * (len(shape) - 1 - dim))
    return level


def bell_draw(stream_key, shape, deviation, reach, pieces=(), kind=jnp.bfloat16):
    drawn = deviation * jax.random.normal(stream_key, shape, jnp.float32)
    if pieces:
        drawn = drawn * block_levels(stream_key, shape, pieces, -0.22, 0.18)
    return jnp.clip(drawn, -reach, reach).astype(kind)


def setup_inputs(seed: int = 0) -> dict:
    streams_of = jax.random.split(jax.random.key(seed), 7)
    features = jnp.clip(2.0 * jax.random.uniform(streams_of[0], (TARGETS, SIDE, SIDE, C), jnp.float32) ** block_levels(streams_of[0], (TARGETS, SIDE, SIDE, C), ((0, 256),), -0.2, 0.2), 0.0, 2.0).astype(jnp.bfloat16)
    labels = with_ends(jax.random.randint(streams_of[1], (TARGETS,), 0, CLASSES), jax.random.fold_in(streams_of[1], 1), 0, CLASSES - 1).astype(jnp.int32)
    subset_ids = with_ends(jax.random.randint(streams_of[2], (MODELS,), 0, SUBSETS), jax.random.fold_in(streams_of[2], 1), 0, SUBSETS - 1).astype(jnp.int32)
    conv1_weight = bell_draw(streams_of[3], (MODELS, 9, C, C), (9 * C) ** -0.5, 0.09375, ((0, 64),))
    conv2_weight = bell_draw(streams_of[4], (MODELS, 9, C, C), (9 * C) ** -0.5, 0.09375, ((0, 64),))
    head_weight = bell_draw(streams_of[5], (MODELS, C, CLASSES), C ** -0.5, 0.25, ((0, 64),), jnp.float32)
    return {"features": features, "labels": labels, "subset_ids": subset_ids, "conv1_weight": conv1_weight, "conv2_weight": conv2_weight, "head_weight": head_weight}


def convolve(grid, kernel):
    batch = grid.shape[0]
    width = grid.shape[1]
    chans = grid.shape[3]
    padded = jnp.pad(grid, ((0, 0), (1, 1), (1, 1), (0, 0)))
    result = jnp.zeros((batch * width * width, kernel.shape[2]), jnp.float32)
    for offset in range(9):
        row_off, col_off = divmod(offset, 3)
        shifted = padded[:, row_off:row_off + width, col_off:col_off + width, :].reshape(batch * width * width, chans)
        result = result + jnp.dot(shifted, kernel[offset], preferred_element_type=jnp.float32)
    return result

def margins_of(grid, first_kernel, second_kernel, head, target_labels):
    batch = grid.shape[0]
    width = grid.shape[1]
    chans = grid.shape[3]
    hidden = jax.nn.relu(convolve(grid, first_kernel)).astype(jnp.bfloat16).reshape(batch, width, width, chans)
    branch = jax.nn.relu(convolve(hidden, second_kernel))
    blocked = grid.astype(jnp.float32).reshape(batch * width * width, chans) + branch
    pooled = lax.optimization_barrier(jnp.max(blocked.reshape(batch, width * width, chans), axis=1))
    logits = jnp.dot(pooled, head, precision=lax.Precision.HIGHEST, preferred_element_type=jnp.float32)
    classes = jnp.arange(head.shape[1], dtype=jnp.int32)[None, :]
    chosen = classes == target_labels[:, None]
    correct = lax.optimization_barrier(jnp.sum(jnp.where(chosen, logits, 0.0), axis=1))
    rival = lax.optimization_barrier(jnp.max(jnp.where(chosen, -1e+30, logits), axis=1))
    return correct - rival

def reference(features, labels, subset_ids, conv1_weight, conv2_weight, head_weight):

    def single(weights):
        return margins_of(features, weights[0], weights[1], weights[2], labels)
    margin = lax.map(single, (conv1_weight, conv2_weight, head_weight))
    model_count = margin.shape[0]
    margin_mean = lax.optimization_barrier(jnp.sum(margin, axis=0)) / model_count
    centred = margin - margin_mean[None, :]
    margin_norm = jnp.sqrt(1.0 + lax.optimization_barrier(jnp.sum(centred * centred, axis=0)) / model_count)
    scaled = centred / margin_norm[None, :]
    onehot = (subset_ids[:, None] == jnp.arange(SUBSETS, dtype=jnp.int32)[None, :]).astype(jnp.float32)
    datamodel = jnp.dot(scaled.T, onehot, precision=lax.Precision.HIGHEST, preferred_element_type=jnp.float32)
    return (datamodel, margin_mean, margin_norm)
```

```python
import functools

import jax
import jax.numpy as jnp
from jax import lax
from jax.experimental import pallas as pl
from jax.experimental.pallas import tpu as pltpu
from jax.sharding import PartitionSpec as P

SUBSETS = 256
LANES = 128
T = 16
TILE = 256
MESH = pl.DeviceIdType.MESH
NY, NZ = 4, 8

BOTH = (0, 1)
NEAR = [(0, 0), (0, 1), (0, -1), (1, 0), (-1, 0), (0, 2), (0, -2), (2, 0)]
CHUNKS = [
    [(y, z, 0) for y, z in NEAR] + [(y, z, 1) for y, z in NEAR],
    [(0, z, c) for z in (3, -3, 4) for c in BOTH]
    + [(y, z, c) for z in (1, -1) for y in (1, -1) for c in BOTH]
    + [(1, 2, 0), (-1, 2, 0)],
    [(1, 2, 1), (-1, 2, 1)]
    + [(y, z, c) for z in (-2, 3, -3) for y in (1, -1) for c in BOTH]
    + [(1, 4, 0), (-1, 4, 0)],
    [(1, 4, 1), (-1, 4, 1)] + [(2, z, c) for z in (1, -1, 2, -2, 3, -3, 4) for c in BOTH],
]


def norm(r):
    dy, dz, dc = r
    dy, dz = dy % NY, dz % NZ
    return (dy - NY if dy > NY // 2 else dy, dz - NZ if dz > NZ // 2 else dz, dc % 2)


SLOT = {norm(r): i for i, r in enumerate(sum(CHUNKS, []))}
REL = {i: r for r, i in SLOT.items()}
assert len(SLOT) == NY * NZ * 2


def minus(r, d):
    return norm((r[0] - d[0], r[1] - d[1], (r[2] + d[2]) % 2))


SIB, UP, DOWN, FAR = (0, 0, 1), (1, 0, 0), (-1, 0, 0), (2, 0, 0)
ZS = [(0, z, 0) for z in (4, 3, -3, 2, -2, 1, -1)]
PEERS = ZS + [FAR, UP, DOWN, SIB]


def kernel(
    n, feat_ref, labels_ref, ids_ref, w1_ref, w2_ref, head_ref,
    got,
    gathered, labels, ids, w1, w2, head, perm, grids, hids, msg,
    small_sem, own_sem, w1_sem, w2_sem, head_sem, fsend, frecv, msend, mrecv,
):
    me = lax.axis_index("mp")
    my = lax.div(me, 2 * NZ)
    mz = lax.rem(lax.div(me, 2), NZ)
    mc = lax.rem(me, 2)
    width = feat_ref.shape[1]
    chans = feat_ref.shape[3]
    spots = width * width
    rows = T * spots
    offsets = w1_ref.shape[1]
    classes = head_ref.shape[0]
    halves = chans // TILE

    def at(r):
        y = lax.rem(my + (r[0] % NY), NY)
        z = lax.rem(mz + (r[1] % NZ), NZ)
        c = mc if r[2] == 0 else 1 - mc
        return (y * NZ + z) * 2 + c

    own = pltpu.make_async_copy(feat_ref.at[0], gathered.at[SLOT[0, 0, 0]], own_sem)
    own.start()
    barrier = pltpu.get_barrier_semaphore()
    for r in PEERS:
        pl.semaphore_signal(barrier, inc=1, device_id={"mp": at(r)}, device_id_type=MESH)
    w1_copies = [pltpu.make_async_copy(w1_ref.at[0, o], w1.at[o], w1_sem.at[o]) for o in range(offsets)]
    w2_copies = [pltpu.make_async_copy(w2_ref.at[0, o], w2.at[o], w2_sem.at[o]) for o in range(offsets)]
    head_copy = pltpu.make_async_copy(head_ref, head, head_sem)
    small_copies = [
        pltpu.make_async_copy(labels_ref, labels, small_sem.at[0]),
        pltpu.make_async_copy(ids_ref, ids, small_sem.at[1]),
    ]
    for copy in small_copies + w1_copies + w2_copies + [head_copy]:
        copy.start()

    r_ = lax.broadcasted_iota(jnp.int32, (rows, rows), 0)
    c_ = lax.broadcasted_iota(jnp.int32, (rows, rows), 1)
    source = lax.rem(r_, T) * spots + lax.div(r_, T)
    perm[...] = jnp.where(c_ == source, 1.0, 0.0)

    sends = []

    def send(r, d):
        s = SLOT[norm(r)]
        there = SLOT[minus(r, d)]
        copy = pltpu.make_async_remote_copy(
            src_ref=gathered.at[s], dst_ref=gathered.at[there],
            send_sem=fsend.at[len(sends)], recv_sem=frecv.at[there],
            device_id={"mp": at(d)}, device_id_type=MESH,
        )
        copy.start()
        sends.append(copy)

    here = {(0, 0, 0)}

    def arrive(r):
        r = norm(r)
        if r in here:
            return
        here.add(r)
        s = SLOT[r]
        pltpu.make_async_remote_copy(
            src_ref=gathered.at[s], dst_ref=gathered.at[s],
            send_sem=fsend.at[0], recv_sem=frecv.at[s],
            device_id={"mp": at(r)}, device_id_type=MESH,
        ).wait_recv()

    def pass_on(r, *where):
        arrive(r)
        for d in where:
            send(r, d)

    def body(accs):
        def conv(stage, lhs, first, tiles):
            ring = accs[stage % len(accs)]
            for i, (rhs, pairs, depth) in enumerate(tiles):
                reg = i % 2
                for q in range(2):
                    pltpu.matmul_push_rhs(rhs(q), staging_register=reg, mxu_index=q)
                for j, (p, s) in enumerate(pairs):
                    x = lhs(s, depth)
                    for q in range(2):
                        pltpu.matmul_acc_lhs(ring[q][p], x, load_staged_rhs=reg if j == 0 else None)

        def conv_tiles(kernel_ref):
            tiles = []
            for o in range(offsets):
                dy, dx = o // 3 - 1, o % 3 - 1
                pairs = [
                    (y * width + x, (y + dy) * width + x + dx)
                    for y in range(width)
                    for x in range(width)
                    if 0 <= y + dy < width and 0 <= x + dx < width
                ]
                for k in range(halves):
                    tiles.append((
                        lambda q, o=o, k=k: kernel_ref[o, k * TILE : (k + 1) * TILE, q * TILE : (q + 1) * TILE],
                        pairs, k,
                    ))
            return tiles

        def drain(stage):
            ring = accs[stage % len(accs)]
            for p in range(spots):
                for q in range(2):
                    yield p, q, pltpu.matmul_pop(ring[q][p])

        def arrange(stage, g):
            raw = gathered[g * T : (g + 1) * T].reshape(rows, chans)
            conv(
                stage,
                lambda s, k: perm[s * T : (s + 1) * T, :],
                None,
                [(lambda q: raw[:, q * TILE : (q + 1) * TILE], [(p, p) for p in range(spots)], 0)],
            )
            for p, q, value in drain(stage):
                grids[g, p * T : (p + 1) * T, q * TILE : (q + 1) * TILE] = value

        def conv1(stage, g):
            conv(stage, lambda s, k: grids[g, s * T : (s + 1) * T, k * TILE : (k + 1) * TILE], None, conv_tiles(w1))
            for p, q, value in drain(stage):
                hids[g, p * T : (p + 1) * T, q * TILE : (q + 1) * TILE] = jnp.maximum(value, 0.0)

        def conv2(stage, g):
            conv(stage, lambda s, k: hids[g, s * T : (s + 1) * T, k * TILE : (k + 1) * TILE], None, conv_tiles(w2))
            pooled = [None] * 2
            for p, q, value in drain(stage):
                block = grids[g, p * T : (p + 1) * T, q * TILE : (q + 1) * TILE] + jnp.maximum(value, 0.0)
                pooled[q] = block if p == 0 else jnp.maximum(pooled[q], block)
            return pooled

        sub = lax.broadcasted_iota(jnp.int32, (T, 1), 0)
        lane = lax.broadcasted_iota(jnp.int32, (T, LANES), 1)

        def margins(g, pooled):
            label = jnp.zeros((T, 1), jnp.int32)
            for t in range(T):
                label = jnp.where(sub == t, labels[at(REL[g * T + t])], label)
            correct = jnp.zeros((T, 1), jnp.float32)
            rival = jnp.full((T, 1), -1e30, jnp.float32)
            for k in range(classes):
                logit = jnp.sum(
                    pooled[0] * head[k, :, :TILE] + pooled[1] * head[k, :, TILE:], axis=1, keepdims=True
                )
                correct = jnp.where(label == k, logit, correct)
                rival = jnp.where(label == k, rival, jnp.maximum(rival, logit))
            identity = ids[0].astype(jnp.float32)
            msg[g * T : (g + 1) * T, :] = jnp.where(lane < LANES // 2, correct - rival, identity)
            for t in range(T):
                s = g * T + t
                r = REL[s]
                if r == (0, 0, 0):
                    got[0:1, :] = msg[s : s + 1, :]
                    continue
                there = SLOT[minus((0, 0, 0), r)]
                copy = pltpu.make_async_remote_copy(
                    src_ref=msg.at[pl.ds(s, 1)], dst_ref=got.at[pl.ds(there, 1)],
                    send_sem=msend.at[s], recv_sem=mrecv.at[there],
                    device_id={"mp": at(r)}, device_id_type=MESH,
                )
                copy.start()
                margin_sends.append(copy)

        margin_sends = []
        for ring in accs:
            for q in range(2):
                for p in range(spots):
                    pltpu.matmul_pop(ring[q][p])
        own.wait()
        pl.semaphore_wait(barrier, len(PEERS))
        for d in PEERS:
            send((0, 0, 0), d)
        for z in (1, -1):
            pass_on((0, z, 0), UP, DOWN, SIB)
        pass_on((1, 0, 0), SIB)
        pass_on((-1, 0, 0), SIB)
        for z in (2, -2):
            pass_on((0, z, 0), UP, DOWN, SIB)
        pass_on((2, 0, 0), SIB)
        for z in (3, -3):
            pass_on((0, z, 0), UP, DOWN, SIB)

        def ready(g):
            for r in CHUNKS[g]:
                arrive(r)

        for copy in small_copies:
            copy.wait()
        ready(0)
        arrange(0, 0)
        for copy in w1_copies:
            copy.wait()
        conv1(1, 0)

        pass_on((0, 4, 0), UP, DOWN, SIB)
        for z in (1, 2):
            pass_on((1, z, 0), SIB, DOWN)
            pass_on((-1, z, 0), SIB)
        for z in (-1, -2):
            pass_on((1, z, 0), SIB)
            pass_on((-1, z, 0), SIB, UP)
        for copy in w2_copies:
            copy.wait()
        head_copy.wait()
        pooled0 = conv2(2, 0)

        pass_on((1, 3, 0), SIB, DOWN)
        pass_on((-1, 3, 0), SIB)
        pass_on((1, -3, 0), SIB)
        pass_on((-1, -3, 0), SIB, UP)
        ready(1)
        arrange(3, 1)
        margins(0, pooled0)
        conv1(4, 1)

        pass_on((1, 4, 0), SIB, DOWN)
        pass_on((-1, 4, 0), SIB)
        ready(2)
        arrange(5, 2)
        conv1(6, 2)

        for z in (1, -1, 2, -2, 3, -3):
            pass_on((2, z, 0), SIB)
        pooled1 = conv2(7, 1)

        pass_on((2, 4, 0), SIB)
        margins(1, pooled1)
        pooled2 = conv2(8, 2)

        ready(3)
        arrange(9, 3)
        margins(2, pooled2)
        conv1(10, 3)
        margins(3, conv2(11, 3))

        for copy in sends:
            copy.wait_send()
        for copy in margin_sends:
            copy.wait_send()
        for s in range(n):
            if s != SLOT[0, 0, 0]:
                pltpu.make_async_remote_copy(
                    src_ref=msg.at[pl.ds(s, 1)], dst_ref=got.at[pl.ds(s, 1)],
                    send_sem=msend.at[0], recv_sem=mrecv.at[s],
                    device_id={"mp": at(REL[s])}, device_id_type=MESH,
                ).wait_recv()

    acc = lambda q: pltpu.ACC(q)((T, TILE), jnp.float32)
    pl.run_scoped(body, tuple(tuple(tuple(acc(q) for _ in range(spots)) for q in range(2)) for _ in range(4)))


def finish(got, data_ref, mean_ref, norm_ref):
    n = got.shape[0]
    half = LANES // 2
    lane = lax.broadcasted_iota(jnp.int32, (n, LANES), 1)
    both = got[...]
    swapped = pltpu.roll(both, half, 1)
    margin = jnp.where(lane < half, both, swapped)
    identity = jnp.where(lane < half, swapped, both)
    mean = jnp.sum(margin, axis=0, keepdims=True) / n
    centred = margin - mean
    norm_ = jnp.sqrt(1.0 + jnp.sum(centred * centred, axis=0, keepdims=True) / n)
    scaled = centred / norm_
    for start in range(0, SUBSETS, LANES):
        here = identity == (lane + start).astype(jnp.float32)
        data_ref[:, start : start + LANES] = jnp.sum(jnp.where(here, scaled, 0.0), axis=0, keepdims=True)
    mean_ref[...] = mean[0, :1]
    norm_ref[...] = norm_[0, :1]


def shards(n, features, labels, subset_ids, conv1_weight, conv2_weight, head_weight):
    width, chans = features.shape[1], features.shape[3]
    offsets = conv1_weight.shape[1]
    spots = width * width
    assert features.shape[0] == 1 and conv1_weight.shape[0] == 1 and n == NY * NZ * 2
    features = features.reshape(1, spots, chans) if False else features
    head = jnp.transpose(head_weight, (2, 0, 1))
    anywhere = pl.BlockSpec(memory_space=pl.ANY)
    hbm = pl.BlockSpec(memory_space=pltpu.HBM)
    vmem = pl.BlockSpec(memory_space=pltpu.VMEM)
    chunks = n // T
    got = pl.pallas_call(
        functools.partial(kernel, n),
        out_shape=pltpu.VMEM((n, LANES), jnp.float32),
        in_specs=[anywhere, hbm, hbm, anywhere, anywhere, anywhere],
        out_specs=vmem,
        scratch_shapes=[
            pltpu.VMEM((n, width, width, chans), features.dtype),
            pltpu.SMEM(labels.shape, labels.dtype),
            pltpu.SMEM(subset_ids.shape, subset_ids.dtype),
            pltpu.VMEM(conv1_weight.shape[1:], conv1_weight.dtype),
            pltpu.VMEM(conv2_weight.shape[1:], conv2_weight.dtype),
            pltpu.VMEM(head.shape, head.dtype),
            pltpu.VMEM((T * spots, T * spots), jnp.float32),
            pltpu.VMEM((chunks, T * spots, chans), jnp.float32),
            pltpu.VMEM((chunks, T * spots, chans), jnp.float32),
            pltpu.VMEM((n, LANES), jnp.float32),
            pltpu.SemaphoreType.DMA((2,)),
            pltpu.SemaphoreType.DMA,
            pltpu.SemaphoreType.DMA((offsets,)),
            pltpu.SemaphoreType.DMA((offsets,)),
            pltpu.SemaphoreType.DMA,
            pltpu.SemaphoreType.DMA((80,)),
            pltpu.SemaphoreType.DMA((n,)),
            pltpu.SemaphoreType.DMA((n,)),
            pltpu.SemaphoreType.DMA((n,)),
        ],
        compiler_params=pltpu.CompilerParams(
            collective_id=0, has_side_effects=True, vmem_limit_bytes=60 * 1024 * 1024
        ),
    )(features, labels, subset_ids, conv1_weight, conv2_weight, head)
    return pl.pallas_call(
        finish,
        out_shape=(
            jax.ShapeDtypeStruct((1, SUBSETS), jnp.float32),
            jax.ShapeDtypeStruct((1,), jnp.float32),
            jax.ShapeDtypeStruct((1,), jnp.float32),
        ),
        in_specs=[vmem],
        out_specs=(vmem, vmem, vmem),
    )(pltpu.with_memory_space_constraint(got, pltpu.VMEM))


def solution(mesh):
    in_specs = (
        P(("dp", "mp"), None, None, None),
        P("dp"),
        P("mp"),
        P("mp", None, None, None),
        P("mp", None, None, None),
        P("mp", None, None),
    )
    out_specs = (P(("dp", "mp"), None), P(("dp", "mp")), P(("dp", "mp")))
    return jax.shard_map(
        functools.partial(shards, mesh.shape["mp"]),
        mesh=mesh, in_specs=in_specs, out_specs=out_specs, check_vma=False,
    )
```

```python
import functools

import jax
import jax.numpy as jnp
from jax import lax
from jax.experimental import pallas as pl
from jax.experimental.pallas import tpu as pltpu
from jax.sharding import PartitionSpec as P

SUBSETS = 256
LANES = 128
TILE = 256
MESH = pl.DeviceIdType.MESH
NY, NZ = 4, 8
BOTH = (1, -1)

CHUNKS = [
    [(y, z, c) for c in (0, 1) for y, z in ((0, 0), (0, 1), (0, -1), (1, 0), (-1, 0), (0, 2), (0, -2), (2, 0))],
    [(y, z, 0) for y in BOTH for z in BOTH]
    + [(2, 1, 0), (2, -1, 0)]
    + [(y, 2 * z, 0) for y in BOTH for z in BOTH]
    + [(y, z, 1) for y in BOTH for z in BOTH]
    + [(2, 1, 1), (2, -1, 1)],
    [(2, 2, 0), (2, -2, 0), (0, 3, 0), (0, -3, 0), (0, 4, 0), (1, 3, 0), (-1, 3, 0)]
    + [(y, 2 * z, 1) for y in BOTH for z in BOTH]
    + [(2, 2, 1), (2, -2, 1), (0, 3, 1), (0, -3, 1), (0, 4, 1)],
    [(y, z, 0) for y, z in ((1, -3), (-1, -3), (2, 3), (2, -3), (1, 4), (-1, 4), (2, 4))]
    + [(y, z, 1) for y, z in ((1, -3), (-1, -3), (2, 3), (2, -3), (1, 4), (-1, 4), (2, 4), (1, 3), (-1, 3))],
]
STARTS = [sum(map(len, CHUNKS[:g])) for g in range(len(CHUNKS))]


def norm(r):
    dy, dz, dc = r
    dy, dz = dy % NY, dz % NZ
    return (dy - NY if dy > NY // 2 else dy, dz - NZ if dz > NZ // 2 else dz, dc % 2)


REL = sum(CHUNKS, [])
SLOT = {norm(r): i for i, r in enumerate(REL)}
CHUNK_OF = {norm(r): g for g, chunk in enumerate(CHUNKS) for r in chunk}
assert len(SLOT) == len(REL) == NY * NZ * 2


def minus(r, d):
    return norm((r[0] - d[0], r[1] - d[1], (r[2] + d[2]) % 2))


SIB, UP, DOWN, FAR = (0, 0, 1), (1, 0, 0), (-1, 0, 0), (2, 0, 0)
COLUMN = [FAR, UP, DOWN]
NEXT = [SIB, (0, 1, 0), (0, -1, 0), UP, DOWN, (0, 2, 0), (0, -2, 0), FAR]
SENDS = 63


def kernel(
    n, feat_ref, labels_ref, ids_ref, w1_ref, w2_ref, head_ref,
    got,
    gathered, labels, ids, w1, w2, head, grids, hids, msg,
    mid, small_sem, own_sem, w1_sem, w2_sem, head_sem, fsend, frecv, grecv, msend, mrecv,
):
    me = lax.axis_index("mp")
    my = lax.div(me, 2 * NZ)
    mz = lax.rem(lax.div(me, 2), NZ)
    mc = lax.rem(me, 2)
    width = feat_ref.shape[1]
    chans = feat_ref.shape[3]
    spots = width * width
    offsets = w1_ref.shape[1]
    classes = head_ref.shape[0]
    halves = chans // TILE

    def at(r):
        y = lax.rem(my + (r[0] % NY), NY)
        z = lax.rem(mz + (r[1] % NZ), NZ)
        c = mc if r[2] == 0 else 1 - mc
        return (y * NZ + z) * 2 + c

    own = pltpu.make_async_copy(feat_ref.at[0], gathered.at[0], own_sem)
    own.start()
    barrier = pltpu.get_barrier_semaphore()
    for r in NEXT:
        pl.semaphore_signal(barrier, inc=1, device_id={"mp": at(r)}, device_id_type=MESH)
    small_copies = [
        pltpu.make_async_copy(labels_ref, labels, small_sem.at[0]),
        pltpu.make_async_copy(ids_ref, ids, small_sem.at[1]),
    ]
    for copy in small_copies:
        copy.start()
    for o in range(offsets):
        pltpu.make_async_copy(w1_ref.at[0, o], w1.at[o], w1_sem).start()
    for o in range(offsets):
        pltpu.make_async_copy(w2_ref.at[0, o], w2.at[o], w2_sem).start()
    head_copy = pltpu.make_async_copy(head_ref, head, head_sem)
    head_copy.start()

    sent = []

    def send(r, d):
        s = SLOT[norm(r)]
        source = minus(r, d)
        there = SLOT[source]
        pltpu.make_async_remote_copy(
            src_ref=gathered.at[s], dst_ref=gathered.at[there],
            send_sem=fsend, recv_sem=grecv.at[CHUNK_OF[source]] if source[2] else frecv.at[there],
            device_id={"mp": at(d)}, device_id_type=MESH,
        ).start()
        sent.append(d)

    here = {(0, 0, 0)}

    def arrive(r):
        r = norm(r)
        if r in here:
            return
        here.add(r)
        s = SLOT[r]
        pltpu.make_async_copy(gathered.at[s], gathered.at[s], frecv.at[s]).wait()

    def pass_on(r, *where):
        arrive(r)
        for d in where:
            send(r, d)

    def ready(g):
        others = [r for r in CHUNKS[g] if r[2]]
        for r in CHUNKS[g]:
            if not r[2]:
                arrive(r)
        block = gathered.at[pl.ds(SLOT[norm(others[0])], len(others))]
        pltpu.make_async_copy(block, block, grecv.at[g]).wait()

    def body(rings):
        turns = []

        def take(t):
            turns.append(t)
            return rings[(len(turns) - 1) % len(rings)]

        def multiply(ring, lhs, tiles, between={}):
            for i, (rhs, pairs, depth) in enumerate(tiles):
                reg = i % 2
                for q in range(2):
                    pltpu.matmul_push_rhs(rhs(q), staging_register=reg, mxu_index=q)
                for j, (p, s) in enumerate(pairs):
                    x = lhs(s, depth)
                    for q in range(2):
                        pltpu.matmul_acc_lhs(ring[q][p], x, load_staged_rhs=reg if j == 0 else None)
                if i in between:
                    between[i]()

        def conv_tiles(kernel_ref):
            tiles = []
            for o in range(offsets):
                dy, dx = o // 3 - 1, o % 3 - 1
                pairs = [
                    (y * width + x, (y + dy) * width + x + dx)
                    for y in range(width)
                    for x in range(width)
                    if 0 <= y + dy < width and 0 <= x + dx < width
                ]
                for k in range(halves):
                    tiles.append((
                        lambda q, o=o, k=k: kernel_ref[o, k * TILE : (k + 1) * TILE, q * TILE : (q + 1) * TILE],
                        pairs, k,
                    ))
            return tiles

        def drain(ring):
            for p in range(spots):
                for q in range(2):
                    yield p, q, pltpu.matmul_pop(ring[q][p])

        def place(g, p, k):
            t = len(CHUNKS[g])
            first = STARTS[g] * spots + p * t
            return (slice(first, first + t), slice(k * TILE, (k + 1) * TILE))

        def arrange(g):
            t = len(CHUNKS[g])
            ring = take(t)
            raw = gathered[STARTS[g] : STARTS[g] + t].reshape(t * spots, chans)
            if t * spots < TILE:
                raw = jnp.concatenate([raw, jnp.zeros((TILE - t * spots, chans), raw.dtype)], 0)
            row = lax.broadcasted_iota(jnp.int32, (t, TILE), 0)
            col = lax.broadcasted_iota(jnp.int32, (t, TILE), 1)
            multiply(
                ring,
                lambda s, k: jnp.where(col == row * spots + s, 1.0, 0.0),
                [(lambda q: raw[:, q * TILE : (q + 1) * TILE], [(p, p) for p in range(spots)], 0)],
            )
            return ring

        def arranged(g, ring):
            for p, q, value in drain(ring):
                grids[place(g, p, q)] = value

        def conv1(g, between={}):
            ring = take(len(CHUNKS[g]))
            multiply(ring, lambda s, k: grids[place(g, s, k)], conv_tiles(w1), between)
            return ring

        def conv1d(g, ring):
            for p, q, value in drain(ring):
                hids[place(g, p, q)] = jnp.maximum(value, 0.0)

        def conv2(g, between={}):
            ring = take(len(CHUNKS[g]))
            multiply(ring, lambda s, k: hids[place(g, s, k)], conv_tiles(w2), between)
            return ring

        def conv2d(g, ring):
            pooled = [None] * 2
            for p, q, value in drain(ring):
                block = grids[place(g, p, q)] + jnp.maximum(value, 0.0)
                pooled[q] = block if p == 0 else jnp.maximum(pooled[q], block)
            return pooled

        def margins(g, pooled):
            t = len(CHUNKS[g])
            sub = lax.broadcasted_iota(jnp.int32, (t, 1), 0)
            lane = lax.broadcasted_iota(jnp.int32, (t, LANES), 1)
            label = jnp.zeros((t, 1), jnp.int32)
            for i, r in enumerate(CHUNKS[g]):
                label = jnp.where(sub == i, labels[at(r)], label)
            correct = jnp.zeros((t, 1), jnp.float32)
            rival = jnp.full((t, 1), -1e30, jnp.float32)
            for k in range(classes):
                logit = jnp.sum(
                    pooled[0] * head[k, :, :TILE] + pooled[1] * head[k, :, TILE:], axis=1, keepdims=True
                )
                correct = jnp.where(label == k, logit, correct)
                rival = jnp.where(label == k, rival, jnp.maximum(rival, logit))
            identity = ids[0].astype(jnp.float32)
            first = STARTS[g]
            msg[first : first + t, :] = jnp.where(lane < LANES // 2, correct - rival, identity)
            for i, r in enumerate(CHUNKS[g]):
                s = first + i
                if r == (0, 0, 0):
                    got[0:1, :] = msg[0:1, :]
                    continue
                there = SLOT[minus((0, 0, 0), r)]
                pltpu.make_async_remote_copy(
                    src_ref=msg.at[pl.ds(s, 1)], dst_ref=got.at[pl.ds(there, 1)],
                    send_sem=msend, recv_sem=mrecv,
                    device_id={"mp": at(r)}, device_id_type=MESH,
                ).start()

        for ring in rings:
            for q in range(2):
                for p in range(spots):
                    pltpu.matmul_pop(ring[q][p])
        pl.semaphore_wait(barrier, len(NEXT))
        for i, z in enumerate((2, -2)):
            pl.semaphore_signal(mid.at[i], inc=1, device_id={"mp": at((0, z, 0))}, device_id_type=MESH)
        own.wait()
        for d in NEXT:
            send((0, 0, 0), d)
        for i in range(2):
            pl.semaphore_wait(mid.at[i], 1)
        for z in (3, -3, 4):
            send((0, 0, 0), (0, z, 0))
        for z in BOTH:
            pass_on((0, z, 0), SIB, *COLUMN)
        for y in BOTH:
            pass_on((y, 0, 0), SIB)
        for z in BOTH:
            pass_on((0, 2 * z, 0), SIB, *COLUMN)
        pass_on((2, 0, 0), SIB)
        for copy in small_copies:
            copy.wait()
        pltpu.make_async_copy(w1, w1, w1_sem).wait()
        pltpu.make_async_copy(w2, w2, w2_sem).wait()
        head_copy.wait()
        ready(0)
        arranged(0, arrange(0))

        def ones():
            for y in BOTH:
                for z in BOTH:
                    pass_on((y, z, 0), SIB)

        def threes():
            for z in BOTH:
                pass_on((0, 3 * z, 0), *COLUMN, SIB)
            for z in BOTH:
                pass_on((2, z, 0), SIB)

        def four():
            pass_on((0, 4, 0), *COLUMN, *[(y, 0, 1) for y, _, _ in COLUMN], SIB)
            for z in BOTH:
                pass_on((2, 2 * z, 0), SIB)

        first = conv1(0, {5: ones, 11: threes})
        for y in BOTH:
            for z in BOTH:
                pass_on((y, 2 * z, 0), SIB)
        conv1d(0, first)
        second = conv2(0, {11: four})
        ready(1)
        arrange1 = arrange(1)
        pooled0 = conv2d(0, second)
        arranged(1, arrange1)

        def last():
            for y in BOTH:
                for z in BOTH:
                    pass_on((y, 3 * z, 0), SIB)
            for z in BOTH:
                pass_on((2, 3 * z, 0), SIB)

        first1 = conv1(1, {15: last})
        margins(0, pooled0)
        ready(2)
        arrange2 = arrange(2)
        conv1d(1, first1)
        arranged(2, arrange2)
        first2 = conv1(2)
        second1 = conv2(1)
        conv1d(2, first2)
        ready(3)
        arrange3 = arrange(3)
        pooled1 = conv2d(1, second1)
        arranged(3, arrange3)
        first3 = conv1(3)
        margins(1, pooled1)
        second2 = conv2(2)
        conv1d(3, first3)
        pooled2 = conv2d(2, second2)
        second3 = conv2(3)
        margins(2, pooled2)
        margins(3, conv2d(3, second3))

        assert len(sent) == SENDS
        pltpu.make_async_copy(gathered.at[pl.ds(0, SENDS)], gathered.at[pl.ds(0, SENDS)], fsend).wait()
        pltpu.make_async_copy(msg.at[pl.ds(1, n - 1)], msg.at[pl.ds(1, n - 1)], msend).wait()
        pltpu.make_async_copy(got.at[pl.ds(1, n - 1)], got.at[pl.ds(1, n - 1)], mrecv).wait()

    def rings(count, t):
        return tuple(
            tuple(tuple(pltpu.ACC(q)((t, TILE), jnp.float32) for _ in range(spots)) for q in range(2))
            for _ in range(count)
        )

    pl.run_scoped(body, rings(4, 16))


def finish(got, data_ref, mean_ref, norm_ref):
    n = got.shape[0]
    half = LANES // 2
    lane = lax.broadcasted_iota(jnp.int32, (n, LANES), 1)
    both = got[...]
    swapped = pltpu.roll(both, half, 1)
    margin = jnp.where(lane < half, both, swapped)
    identity = jnp.where(lane < half, swapped, both)
    mean = jnp.sum(margin, axis=0, keepdims=True) / n
    centred = margin - mean
    norm_ = jnp.sqrt(1.0 + jnp.sum(centred * centred, axis=0, keepdims=True) / n)
    scaled = centred / norm_
    for start in range(0, SUBSETS, LANES):
        here = identity == (lane + start).astype(jnp.float32)
        data_ref[:, start : start + LANES] = jnp.sum(jnp.where(here, scaled, 0.0), axis=0, keepdims=True)
    mean_ref[...] = mean[0, :1]
    norm_ref[...] = norm_[0, :1]


def shards(n, features, labels, subset_ids, conv1_weight, conv2_weight, head_weight):
    width, chans = features.shape[1], features.shape[3]
    offsets = conv1_weight.shape[1]
    spots = width * width
    assert features.shape[0] == 1 and conv1_weight.shape[0] == 1 and n == NY * NZ * 2
    head = jnp.transpose(head_weight, (2, 0, 1))
    anywhere = pl.BlockSpec(memory_space=pl.ANY)
    hbm = pl.BlockSpec(memory_space=pltpu.HBM)
    vmem = pl.BlockSpec(memory_space=pltpu.VMEM)
    got = pl.pallas_call(
        functools.partial(kernel, n),
        out_shape=pltpu.VMEM((n, LANES), jnp.float32),
        in_specs=[anywhere, hbm, hbm, anywhere, anywhere, anywhere],
        out_specs=vmem,
        scratch_shapes=[
            pltpu.VMEM((n, width, width, chans), features.dtype),
            pltpu.SMEM(labels.shape, labels.dtype),
            pltpu.SMEM(subset_ids.shape, subset_ids.dtype),
            pltpu.VMEM(conv1_weight.shape[1:], conv1_weight.dtype),
            pltpu.VMEM(conv2_weight.shape[1:], conv2_weight.dtype),
            pltpu.VMEM(head.shape, head.dtype),
            pltpu.VMEM((n * spots, chans), jnp.float32),
            pltpu.VMEM((n * spots, chans), jnp.float32),
            pltpu.VMEM((n, LANES), jnp.float32),
            pltpu.SemaphoreType.REGULAR((2,)),
            pltpu.SemaphoreType.DMA((2,)),
            pltpu.SemaphoreType.DMA,
            pltpu.SemaphoreType.DMA,
            pltpu.SemaphoreType.DMA,
            pltpu.SemaphoreType.DMA,
            pltpu.SemaphoreType.DMA,
            pltpu.SemaphoreType.DMA((n,)),
            pltpu.SemaphoreType.DMA((len(CHUNKS),)),
            pltpu.SemaphoreType.DMA,
            pltpu.SemaphoreType.DMA,
        ],
        compiler_params=pltpu.CompilerParams(
            collective_id=0, has_side_effects=True, vmem_limit_bytes=60 * 1024 * 1024
        ),
    )(features, labels, subset_ids, conv1_weight, conv2_weight, head)
    return pl.pallas_call(
        finish,
        out_shape=(
            jax.ShapeDtypeStruct((1, SUBSETS), jnp.float32),
            jax.ShapeDtypeStruct((1,), jnp.float32),
            jax.ShapeDtypeStruct((1,), jnp.float32),
        ),
        in_specs=[vmem],
        out_specs=(vmem, vmem, vmem),
    )(pltpu.with_memory_space_constraint(got, pltpu.VMEM))


def solution(mesh):
    in_specs = (
        P(("dp", "mp"), None, None, None),
        P("dp"),
        P("mp"),
        P("mp", None, None, None),
        P("mp", None, None, None),
        P("mp", None, None),
    )
    out_specs = (P(("dp", "mp"), None), P(("dp", "mp")), P(("dp", "mp")))
    return jax.shard_map(
        functools.partial(shards, mesh.shape["mp"]),
        mesh=mesh, in_specs=in_specs, out_specs=out_specs, check_vma=False,
    )
```

```python
import functools

import jax
import jax.numpy as jnp
from jax import lax
from jax.experimental import pallas as pl
from jax.experimental.pallas import tpu as pltpu
from jax.sharding import PartitionSpec as P

SUBSETS = 256
LANES = 128
TILE = 256
MESH = pl.DeviceIdType.MESH
NY, NZ = 4, 8
BOTH = (1, -1)

CHUNKS = [
    [(y, z, c) for c in (0, 1) for y, z in ((0, 0), (0, 1), (0, -1), (1, 0), (-1, 0), (0, 2), (0, -2), (2, 0))],
    [(y, z, 0) for y in BOTH for z in BOTH]
    + [(2, 1, 0), (2, -1, 0)]
    + [(y, 2 * z, 0) for y in BOTH for z in BOTH]
    + [(0, 3, 0), (0, -3, 0)]
    + [(y, z, 1) for y in BOTH for z in BOTH],
    [(2, 2, 0), (2, -2, 0), (0, 4, 0), (1, 3, 0), (-1, 3, 0), (0, 3, 1), (0, -3, 1), (2, 1, 1), (2, -1, 1)]
    + [(y, 2 * z, 1) for y in BOTH for z in BOTH]
    + [(2, 2, 1), (2, -2, 1), (0, 4, 1)],
    [(y, z, 0) for y, z in ((1, -3), (-1, -3), (2, 3), (2, -3), (1, 4), (-1, 4), (2, 4))]
    + [(y, z, 1) for y, z in ((1, -3), (-1, -3), (2, 3), (2, -3), (1, 4), (-1, 4), (2, 4), (1, 3), (-1, 3))],
]
STARTS = [sum(map(len, CHUNKS[:g])) for g in range(len(CHUNKS))]


def norm(r):
    dy, dz, dc = r
    dy, dz = dy % NY, dz % NZ
    return (dy - NY if dy > NY // 2 else dy, dz - NZ if dz > NZ // 2 else dz, dc % 2)


REL = sum(CHUNKS, [])
SLOT = {norm(r): i for i, r in enumerate(REL)}
CHUNK_OF = {norm(r): g for g, chunk in enumerate(CHUNKS) for r in chunk}
assert len(SLOT) == len(REL) == NY * NZ * 2


def minus(r, d):
    return norm((r[0] - d[0], r[1] - d[1], (r[2] + d[2]) % 2))


SIB, UP, DOWN, FAR = (0, 0, 1), (1, 0, 0), (-1, 0, 0), (2, 0, 0)
COLUMN = [FAR, UP, DOWN]
NEXT = [SIB, (0, 1, 0), (0, -1, 0), UP, DOWN, (0, 2, 0), (0, -2, 0), FAR]
SENDS = 63


def kernel(
    n, feat_ref, labels_ref, ids_ref, w1_ref, w2_ref, head_ref,
    got,
    gathered, labels, ids, w1, w2, head, grids, hids, msg,
    mid, small_sem, own_sem, w1_sem, w2_sem, head_sem, fsend, frecv, grecv, msend, mrecv,
):
    me = lax.axis_index("mp")
    my = lax.div(me, 2 * NZ)
    mz = lax.rem(lax.div(me, 2), NZ)
    mc = lax.rem(me, 2)
    width = feat_ref.shape[1]
    chans = feat_ref.shape[3]
    spots = width * width
    offsets = w1_ref.shape[1]
    classes = head_ref.shape[0]
    halves = chans // TILE

    def at(r):
        y = lax.rem(my + (r[0] % NY), NY)
        z = lax.rem(mz + (r[1] % NZ), NZ)
        c = mc if r[2] == 0 else 1 - mc
        return (y * NZ + z) * 2 + c

    own = pltpu.make_async_copy(feat_ref.at[0], gathered.at[0], own_sem)
    own.start()
    barrier = pltpu.get_barrier_semaphore()
    for r in NEXT:
        pl.semaphore_signal(barrier, inc=1, device_id={"mp": at(r)}, device_id_type=MESH)
    small_copies = [
        pltpu.make_async_copy(labels_ref, labels, small_sem.at[0]),
        pltpu.make_async_copy(ids_ref, ids, small_sem.at[1]),
    ]
    for copy in small_copies:
        copy.start()
    for o in range(offsets):
        pltpu.make_async_copy(w1_ref.at[0, o], w1.at[o], w1_sem).start()
    for o in range(offsets):
        pltpu.make_async_copy(w2_ref.at[0, o], w2.at[o], w2_sem).start()
    head_copy = pltpu.make_async_copy(head_ref, head, head_sem)
    head_copy.start()

    sent = []

    def send(r, d):
        s = SLOT[norm(r)]
        source = minus(r, d)
        there = SLOT[source]
        pltpu.make_async_remote_copy(
            src_ref=gathered.at[s], dst_ref=gathered.at[there],
            send_sem=fsend, recv_sem=grecv.at[CHUNK_OF[source]] if source[2] else frecv.at[there],
            device_id={"mp": at(d)}, device_id_type=MESH,
        ).start()
        sent.append(d)

    here = {(0, 0, 0)}

    def arrive(r):
        r = norm(r)
        if r in here:
            return
        here.add(r)
        s = SLOT[r]
        pltpu.make_async_copy(gathered.at[s], gathered.at[s], frecv.at[s]).wait()

    def pass_on(r, *where):
        arrive(r)
        for d in where:
            send(r, d)

    def ready(g):
        others = [r for r in CHUNKS[g] if r[2]]
        for r in CHUNKS[g]:
            if not r[2]:
                arrive(r)
        block = gathered.at[pl.ds(SLOT[norm(others[0])], len(others))]
        pltpu.make_async_copy(block, block, grecv.at[g]).wait()

    def body(rings):
        turns = []

        def take(t):
            turns.append(t)
            return rings[(len(turns) - 1) % len(rings)]

        def multiply(ring, lhs, tiles, between={}):
            for i, (rhs, pairs, depth) in enumerate(tiles):
                reg = i % 2
                for q in range(2):
                    pltpu.matmul_push_rhs(rhs(q), staging_register=reg, mxu_index=q)
                for j, (p, s) in enumerate(pairs):
                    x = lhs(s, depth)
                    for q in range(2):
                        pltpu.matmul_acc_lhs(ring[q][p], x, load_staged_rhs=reg if j == 0 else None)
                if i in between:
                    between[i]()

        def conv_tiles(kernel_ref):
            tiles = []
            for o in range(offsets):
                dy, dx = o // 3 - 1, o % 3 - 1
                pairs = [
                    (y * width + x, (y + dy) * width + x + dx)
                    for y in range(width)
                    for x in range(width)
                    if 0 <= y + dy < width and 0 <= x + dx < width
                ]
                for k in range(halves):
                    tiles.append((
                        lambda q, o=o, k=k: kernel_ref[o, k * TILE : (k + 1) * TILE, q * TILE : (q + 1) * TILE],
                        pairs, k,
                    ))
            return tiles

        def drain(ring):
            for p in range(spots):
                for q in range(2):
                    yield p, q, pltpu.matmul_pop(ring[q][p])

        def place(g, p, k):
            t = len(CHUNKS[g])
            first = STARTS[g] * spots + p * t
            return (slice(first, first + t), slice(k * TILE, (k + 1) * TILE))

        def arrange(g):
            t = len(CHUNKS[g])
            for i in range(t):
                for y in range(width):
                    first = STARTS[g] * spots + y * width * t + i
                    line = gathered[STARTS[g] + i, y].astype(jnp.float32)
                    for c in range(chans // LANES):
                        grids[c, pl.ds(first, width, stride=t), :] = line[:, c * LANES : (c + 1) * LANES]

        def grid(g, p, k):
            rows = place(g, p, k)[0]
            return jnp.concatenate([grids[c, rows, :] for c in range(k * TILE // LANES, (k + 1) * TILE // LANES)], 1)

        def conv1(g, between={}):
            ring = take(len(CHUNKS[g]))
            multiply(ring, lambda s, k: grid(g, s, k), conv_tiles(w1), between)
            return ring

        def conv1d(g, ring):
            for p, q, value in drain(ring):
                hids[place(g, p, q)] = jnp.maximum(value, 0.0)

        def conv2(g, between={}, ring=None, part=slice(None)):
            ring = ring or take(len(CHUNKS[g]))
            multiply(ring, lambda s, k: hids[place(g, s, k)], conv_tiles(w2)[part], between)
            return ring

        def conv2d(g, ring):
            pooled = [None] * 2
            for p, q, value in drain(ring):
                block = grid(g, p, q) + jnp.maximum(value, 0.0)
                pooled[q] = block if p == 0 else jnp.maximum(pooled[q], block)
            return pooled

        def margins(g, pooled):
            t = len(CHUNKS[g])
            sub = lax.broadcasted_iota(jnp.int32, (t, 1), 0)
            lane = lax.broadcasted_iota(jnp.int32, (t, LANES), 1)
            label = jnp.zeros((t, 1), jnp.int32)
            for i, r in enumerate(CHUNKS[g]):
                label = jnp.where(sub == i, labels[at(r)], label)
            correct = jnp.zeros((t, 1), jnp.float32)
            rival = jnp.full((t, 1), -1e30, jnp.float32)
            for k in range(classes):
                logit = jnp.sum(
                    pooled[0] * head[k, :, :TILE] + pooled[1] * head[k, :, TILE:], axis=1, keepdims=True
                )
                correct = jnp.where(label == k, logit, correct)
                rival = jnp.where(label == k, rival, jnp.maximum(rival, logit))
            identity = ids[0].astype(jnp.float32)
            first = STARTS[g]
            msg[first : first + t, :] = jnp.where(lane < LANES // 2, correct - rival, identity)

        def tell(g):
            first = STARTS[g]
            for i, r in enumerate(CHUNKS[g]):
                s = first + i
                if r == (0, 0, 0):
                    got[0:1, :] = msg[0:1, :]
                    continue
                there = SLOT[minus((0, 0, 0), r)]
                pltpu.make_async_remote_copy(
                    src_ref=msg.at[pl.ds(s, 1)], dst_ref=got.at[pl.ds(there, 1)],
                    send_sem=msend, recv_sem=mrecv,
                    device_id={"mp": at(r)}, device_id_type=MESH,
                ).start()

        for ring in rings:
            for q in range(2):
                for p in range(spots):
                    pltpu.matmul_pop(ring[q][p])
        pl.semaphore_wait(barrier, len(NEXT))
        for i, z in enumerate((2, -2)):
            pl.semaphore_signal(mid.at[i], inc=1, device_id={"mp": at((0, z, 0))}, device_id_type=MESH)
        own.wait()
        for d in NEXT:
            send((0, 0, 0), d)
        for i in range(2):
            pl.semaphore_wait(mid.at[i], 1)
        for z in (3, -3, 4):
            send((0, 0, 0), (0, z, 0))
        for z in BOTH:
            pass_on((0, z, 0), SIB, *COLUMN)
        for y in BOTH:
            pass_on((y, 0, 0), SIB)
        for z in BOTH:
            pass_on((0, 2 * z, 0), SIB, *COLUMN)
        pass_on((2, 0, 0), SIB)
        for copy in small_copies:
            copy.wait()
        pltpu.make_async_copy(w1, w1, w1_sem).wait()
        pltpu.make_async_copy(w2, w2, w2_sem).wait()
        head_copy.wait()
        ready(0)
        arrange(0)

        def four():
            for z in BOTH:
                pass_on((2, z, 0), SIB)
            pass_on((0, 4, 0), *COLUMN, *[(y, 0, 1) for y, _, _ in COLUMN], SIB)

        def two_off():
            for y in BOTH:
                for z in BOTH:
                    pass_on((y, 2 * z, 0), SIB)
            for z in BOTH:
                pass_on((2, 2 * z, 0), SIB)

        def three_off():
            for y in BOTH:
                for z in BOTH:
                    pass_on((y, 3 * z, 0), SIB)
            for z in BOTH:
                pass_on((2, 3 * z, 0), SIB)

        first0 = conv1(0)
        for z in BOTH:
            pass_on((0, 3 * z, 0), *COLUMN, SIB)
        for y in BOTH:
            for z in BOTH:
                pass_on((y, z, 0), SIB)
        conv1d(0, first0)
        second0 = conv2(0, {3: four, 10: two_off})
        ready(1)
        arrange(1)
        first1 = conv1(1)
        pooled0 = conv2d(0, second0)
        margins(0, pooled0)
        conv1d(1, first1)
        second1 = conv2(1, {10: three_off})
        ready(2)
        arrange(2)
        first2 = conv1(2)
        pooled1 = conv2d(1, second1)
        margins(1, pooled1)
        ready(3)
        arrange(3)
        first3 = conv1(3)
        conv1d(2, first2)
        second2 = conv2(2, part=slice(0, 6))
        conv1d(3, first3)
        second3 = conv2(3)

        def far():
            margins(3, conv2d(3, second3))
            tell(3)

        conv2(2, {5: far}, second2, slice(6, None))
        margins(2, conv2d(2, second2))
        for g in (2, 1, 0):
            tell(g)

        assert len(sent) == SENDS
        pltpu.make_async_copy(gathered.at[pl.ds(0, SENDS)], gathered.at[pl.ds(0, SENDS)], fsend).wait()
        pltpu.make_async_copy(msg.at[pl.ds(1, n - 1)], msg.at[pl.ds(1, n - 1)], msend).wait()
        pltpu.make_async_copy(got.at[pl.ds(1, n - 1)], got.at[pl.ds(1, n - 1)], mrecv).wait()

    def rings(count, t):
        return tuple(
            tuple(tuple(pltpu.ACC(q)((t, TILE), jnp.float32) for _ in range(spots)) for q in range(2))
            for _ in range(count)
        )

    pl.run_scoped(body, rings(4, 16))


def finish(got, data_ref, mean_ref, norm_ref):
    n = got.shape[0]
    half = LANES // 2
    lane = lax.broadcasted_iota(jnp.int32, (n, LANES), 1)
    both = got[...]
    swapped = pltpu.roll(both, half, 1)
    margin = jnp.where(lane < half, both, swapped)
    identity = jnp.where(lane < half, swapped, both)
    mean = jnp.sum(margin, axis=0, keepdims=True) / n
    centred = margin - mean
    norm_ = jnp.sqrt(1.0 + jnp.sum(centred * centred, axis=0, keepdims=True) / n)
    scaled = centred / norm_
    for start in range(0, SUBSETS, LANES):
        here = identity == (lane + start).astype(jnp.float32)
        data_ref[:, start : start + LANES] = jnp.sum(jnp.where(here, scaled, 0.0), axis=0, keepdims=True)
    mean_ref[...] = mean[0, :1]
    norm_ref[...] = norm_[0, :1]


def shards(n, features, labels, subset_ids, conv1_weight, conv2_weight, head_weight):
    width, chans = features.shape[1], features.shape[3]
    offsets = conv1_weight.shape[1]
    spots = width * width
    assert features.shape[0] == 1 and conv1_weight.shape[0] == 1 and n == NY * NZ * 2
    head = jnp.transpose(head_weight, (2, 0, 1))
    anywhere = pl.BlockSpec(memory_space=pl.ANY)
    hbm = pl.BlockSpec(memory_space=pltpu.HBM)
    vmem = pl.BlockSpec(memory_space=pltpu.VMEM)
    got = pl.pallas_call(
        functools.partial(kernel, n),
        out_shape=pltpu.VMEM((n, LANES), jnp.float32),
        in_specs=[anywhere, hbm, hbm, anywhere, anywhere, anywhere],
        out_specs=vmem,
        scratch_shapes=[
            pltpu.VMEM((n, width, width, chans), features.dtype),
            pltpu.SMEM(labels.shape, labels.dtype),
            pltpu.SMEM(subset_ids.shape, subset_ids.dtype),
            pltpu.VMEM(conv1_weight.shape[1:], conv1_weight.dtype),
            pltpu.VMEM(conv2_weight.shape[1:], conv2_weight.dtype),
            pltpu.VMEM(head.shape, head.dtype),
            pltpu.VMEM((chans // LANES, n * spots, LANES), jnp.float32),
            pltpu.VMEM((n * spots, chans), jnp.float32),
            pltpu.VMEM((n, LANES), jnp.float32),
            pltpu.SemaphoreType.REGULAR((2,)),
            pltpu.SemaphoreType.DMA((2,)),
            pltpu.SemaphoreType.DMA,
            pltpu.SemaphoreType.DMA,
            pltpu.SemaphoreType.DMA,
            pltpu.SemaphoreType.DMA,
            pltpu.SemaphoreType.DMA,
            pltpu.SemaphoreType.DMA((n,)),
            pltpu.SemaphoreType.DMA((len(CHUNKS),)),
            pltpu.SemaphoreType.DMA,
            pltpu.SemaphoreType.DMA,
        ],
        compiler_params=pltpu.CompilerParams(
            collective_id=0, has_side_effects=True, vmem_limit_bytes=60 * 1024 * 1024
        ),
    )(features, labels, subset_ids, conv1_weight, conv2_weight, head)
    return pl.pallas_call(
        finish,
        out_shape=(
            jax.ShapeDtypeStruct((1, SUBSETS), jnp.float32),
            jax.ShapeDtypeStruct((1,), jnp.float32),
            jax.ShapeDtypeStruct((1,), jnp.float32),
        ),
        in_specs=[vmem],
        out_specs=(vmem, vmem, vmem),
    )(pltpu.with_memory_space_constraint(got, pltpu.VMEM))


def solution(mesh):
    in_specs = (
        P(("dp", "mp"), None, None, None),
        P("dp"),
        P("mp"),
        P("mp", None, None, None),
        P("mp", None, None, None),
        P("mp", None, None),
    )
    out_specs = (P(("dp", "mp"), None), P(("dp", "mp")), P(("dp", "mp")))
    return jax.shard_map(
        functools.partial(shards, mesh.shape["mp"]),
        mesh=mesh, in_specs=in_specs, out_specs=out_specs, check_vma=False,
    )
```

```python
import functools

import jax
import jax.numpy as jnp
from jax import lax
from jax.experimental import pallas as pl
from jax.experimental.pallas import tpu as pltpu
from jax.sharding import PartitionSpec as P

SUBSETS = 256
LANES = 128
TILE = 256
MESH = pl.DeviceIdType.MESH
NY, NZ = 4, 8
BOTH = (1, -1)

CHUNKS = [
    [(y, z, c) for c in (0, 1) for y, z in ((0, 0), (0, 1), (0, -1), (1, 0), (-1, 0), (0, 2), (0, -2), (2, 0))],
    [(y, z, 0) for y in BOTH for z in BOTH]
    + [(2, 1, 0), (2, -1, 0)]
    + [(y, 2 * z, 0) for y in BOTH for z in BOTH]
    + [(0, 3, 0), (0, -3, 0)]
    + [(y, z, 1) for y in BOTH for z in BOTH],
    [(2, 2, 0), (2, -2, 0), (0, 4, 0), (1, 3, 0), (-1, 3, 0), (0, 3, 1), (0, -3, 1), (2, 1, 1), (2, -1, 1)]
    + [(y, 2 * z, 1) for y in BOTH for z in BOTH]
    + [(2, 2, 1), (2, -2, 1), (0, 4, 1)],
    [(y, z, 0) for y, z in ((1, -3), (-1, -3), (2, 3), (2, -3), (1, 4), (-1, 4), (2, 4))]
    + [(y, z, 1) for y, z in ((1, -3), (-1, -3), (2, 3), (2, -3), (1, 4), (-1, 4), (2, 4), (1, 3), (-1, 3))],
]
STARTS = [sum(map(len, CHUNKS[:g])) for g in range(len(CHUNKS))]


def norm(r):
    dy, dz, dc = r
    dy, dz = dy % NY, dz % NZ
    return (dy - NY if dy > NY // 2 else dy, dz - NZ if dz > NZ // 2 else dz, dc % 2)


REL = sum(CHUNKS, [])
SLOT = {norm(r): i for i, r in enumerate(REL)}
CHUNK_OF = {norm(r): g for g, chunk in enumerate(CHUNKS) for r in chunk}
assert len(SLOT) == len(REL) == NY * NZ * 2


def minus(r, d):
    return norm((r[0] - d[0], r[1] - d[1], (r[2] + d[2]) % 2))


SIB, UP, DOWN, FAR = (0, 0, 1), (1, 0, 0), (-1, 0, 0), (2, 0, 0)
COLUMN = [FAR, UP, DOWN]
NEXT = [SIB, (0, 1, 0), (0, -1, 0), UP, DOWN, (0, 2, 0), (0, -2, 0), FAR]
SENDS = 63


def kernel(
    n, feat_ref, labels_ref, ids_ref, w1_ref, w2_ref, head_ref,
    got,
    gathered, labels, ids, w1, w2, head, grids, hids, msg,
    mid, small_sem, own_sem, w1_sem, w2_sem, head_sem, fsend, frecv, grecv, msend, mrecv,
):
    me = lax.axis_index("mp")
    my = lax.div(me, 2 * NZ)
    mz = lax.rem(lax.div(me, 2), NZ)
    mc = lax.rem(me, 2)
    width = feat_ref.shape[1]
    chans = feat_ref.shape[3]
    spots = width * width
    offsets = w1_ref.shape[1]
    classes = head_ref.shape[0]
    halves = chans // TILE

    def at(r):
        y = lax.rem(my + (r[0] % NY), NY)
        z = lax.rem(mz + (r[1] % NZ), NZ)
        c = mc if r[2] == 0 else 1 - mc
        return (y * NZ + z) * 2 + c

    own = pltpu.make_async_copy(feat_ref.at[0], gathered.at[0], own_sem)
    own.start()
    barrier = pltpu.get_barrier_semaphore()
    for r in NEXT:
        pl.semaphore_signal(barrier, inc=1, device_id={"mp": at(r)}, device_id_type=MESH)
    small_copies = [
        pltpu.make_async_copy(labels_ref, labels, small_sem.at[0]),
        pltpu.make_async_copy(ids_ref, ids, small_sem.at[1]),
    ]
    for copy in small_copies:
        copy.start()
    for o in range(offsets):
        pltpu.make_async_copy(w1_ref.at[0, o], w1.at[o], w1_sem).start()
    for o in range(offsets):
        pltpu.make_async_copy(w2_ref.at[0, o], w2.at[o], w2_sem).start()
    head_copy = pltpu.make_async_copy(head_ref, head, head_sem)
    head_copy.start()

    sent = []

    def send(r, d):
        s = SLOT[norm(r)]
        source = minus(r, d)
        there = SLOT[source]
        pltpu.make_async_remote_copy(
            src_ref=gathered.at[s], dst_ref=gathered.at[there],
            send_sem=fsend, recv_sem=grecv.at[CHUNK_OF[source]] if source[2] else frecv.at[there],
            device_id={"mp": at(d)}, device_id_type=MESH,
        ).start()
        sent.append(d)

    here = {(0, 0, 0)}

    def arrive(r):
        r = norm(r)
        if r in here:
            return
        here.add(r)
        s = SLOT[r]
        pltpu.make_async_copy(gathered.at[s], gathered.at[s], frecv.at[s]).wait()

    def pass_on(r, *where):
        arrive(r)
        for d in where:
            send(r, d)

    def ready(g):
        others = [r for r in CHUNKS[g] if r[2]]
        for r in CHUNKS[g]:
            if not r[2]:
                arrive(r)
        block = gathered.at[pl.ds(SLOT[norm(others[0])], len(others))]
        pltpu.make_async_copy(block, block, grecv.at[g]).wait()

    def body(rings):
        turns = []

        def take(t):
            turns.append(t)
            return rings[(len(turns) - 1) % len(rings)]

        def multiply(ring, lhs, tiles, between={}):
            for i, (rhs, pairs, depth) in enumerate(tiles):
                reg = i % 2
                for q in range(2):
                    pltpu.matmul_push_rhs(rhs(q), staging_register=reg, mxu_index=q)
                for j, (p, s) in enumerate(pairs):
                    x = lhs(s, depth)
                    for q in range(2):
                        pltpu.matmul_acc_lhs(ring[q][p], x, load_staged_rhs=reg if j == 0 else None)
                if i in between:
                    between[i]()

        def conv_tiles(kernel_ref):
            tiles = []
            for o in range(offsets):
                dy, dx = o // 3 - 1, o % 3 - 1
                pairs = [
                    (y * width + x, (y + dy) * width + x + dx)
                    for y in range(width)
                    for x in range(width)
                    if 0 <= y + dy < width and 0 <= x + dx < width
                ]
                for k in range(halves):
                    tiles.append((
                        lambda q, o=o, k=k: kernel_ref[o, k * TILE : (k + 1) * TILE, q * TILE : (q + 1) * TILE],
                        pairs, k,
                    ))
            return tiles

        def drain(ring):
            for p in range(spots):
                for q in range(2):
                    yield p, q, pltpu.matmul_pop(ring[q][p])

        def place(g, p, k):
            t = len(CHUNKS[g])
            first = STARTS[g] * spots + p * t
            return (slice(first, first + t), slice(k * TILE, (k + 1) * TILE))

        def arrange(g, span=(16,)):
            t = len(CHUNKS[g])
            for i in range(*span):
                for y in range(width):
                    first = STARTS[g] * spots + y * width * t + i
                    line = gathered[STARTS[g] + i, y].astype(jnp.float32)
                    for c in range(chans // LANES):
                        grids[c, pl.ds(first, width, stride=t), :] = line[:, c * LANES : (c + 1) * LANES]

        def grid(g, p, k):
            rows = place(g, p, k)[0]
            return jnp.concatenate([grids[c, rows, :] for c in range(k * TILE // LANES, (k + 1) * TILE // LANES)], 1)

        def conv1(g, between={}):
            ring = take(len(CHUNKS[g]))
            multiply(ring, lambda s, k: grid(g, s, k), conv_tiles(w1), between)
            return ring

        def conv1d(g, ring):
            for p, q, value in drain(ring):
                hids[place(g, p, q)] = jnp.maximum(value, 0.0)

        def conv2(g, between={}, ring=None, part=slice(None)):
            ring = ring or take(len(CHUNKS[g]))
            multiply(ring, lambda s, k: hids[place(g, s, k)], conv_tiles(w2)[part], between)
            return ring

        def conv2d(g, ring):
            pooled = [None] * 2
            for p, q, value in drain(ring):
                block = grid(g, p, q) + jnp.maximum(value, 0.0)
                pooled[q] = block if p == 0 else jnp.maximum(pooled[q], block)
            return pooled

        def margins(g, pooled):
            t = len(CHUNKS[g])
            sub = lax.broadcasted_iota(jnp.int32, (t, 1), 0)
            lane = lax.broadcasted_iota(jnp.int32, (t, LANES), 1)
            label = jnp.zeros((t, 1), jnp.int32)
            for i, r in enumerate(CHUNKS[g]):
                label = jnp.where(sub == i, labels[at(r)], label)
            correct = jnp.zeros((t, 1), jnp.float32)
            rival = jnp.full((t, 1), -1e30, jnp.float32)
            for k in range(classes):
                logit = jnp.sum(
                    pooled[0] * head[k, :, :TILE] + pooled[1] * head[k, :, TILE:], axis=1, keepdims=True
                )
                correct = jnp.where(label == k, logit, correct)
                rival = jnp.where(label == k, rival, jnp.maximum(rival, logit))
            identity = ids[0].astype(jnp.float32)
            first = STARTS[g]
            msg[first : first + t, :] = jnp.where(lane < LANES // 2, correct - rival, identity)

        def tell(g):
            first = STARTS[g]
            hops = [abs(r[0]) + abs(r[1]) for r in CHUNKS[g]]
            for i in sorted(range(len(hops)), key=lambda i: -hops[i]):
                r = CHUNKS[g][i]
                s = first + i
                if r == (0, 0, 0):
                    got[0:1, :] = msg[0:1, :]
                    continue
                there = SLOT[minus((0, 0, 0), r)]
                pltpu.make_async_remote_copy(
                    src_ref=msg.at[pl.ds(s, 1)], dst_ref=got.at[pl.ds(there, 1)],
                    send_sem=msend, recv_sem=mrecv,
                    device_id={"mp": at(r)}, device_id_type=MESH,
                ).start()

        for ring in rings:
            for q in range(2):
                for p in range(spots):
                    pltpu.matmul_pop(ring[q][p])
        pl.semaphore_wait(barrier, len(NEXT))
        for i, z in enumerate((2, -2)):
            pl.semaphore_signal(mid.at[i], inc=1, device_id={"mp": at((0, z, 0))}, device_id_type=MESH)
        own.wait()
        for d in NEXT:
            send((0, 0, 0), d)
        for i in range(2):
            pl.semaphore_wait(mid.at[i], 1)
        for z in (3, -3, 4):
            send((0, 0, 0), (0, z, 0))
        for z in BOTH:
            pass_on((0, z, 0), SIB, *COLUMN)
        for y in BOTH:
            pass_on((y, 0, 0), SIB)
        for z in BOTH:
            pass_on((0, 2 * z, 0), SIB, *COLUMN)
        pass_on((2, 0, 0), SIB)
        for copy in small_copies:
            copy.wait()
        pltpu.make_async_copy(w1, w1, w1_sem).wait()
        pltpu.make_async_copy(w2, w2, w2_sem).wait()
        head_copy.wait()
        arrange(0, (0, 8))
        ready(0)
        arrange(0, (8, 16))

        def four():
            for z in BOTH:
                pass_on((2, z, 0), SIB)
            pass_on((0, 4, 0), *COLUMN, *[(y, 0, 1) for y, _, _ in COLUMN], SIB)

        def two_off():
            for y in BOTH:
                for z in BOTH:
                    pass_on((y, 2 * z, 0), SIB)
            for z in BOTH:
                pass_on((2, 2 * z, 0), SIB)

        def three_off():
            for y in BOTH:
                for z in BOTH:
                    pass_on((y, 3 * z, 0), SIB)
            for z in BOTH:
                pass_on((2, 3 * z, 0), SIB)

        first0 = conv1(0)
        for z in BOTH:
            pass_on((0, 3 * z, 0), *COLUMN, SIB)
        for y in BOTH:
            for z in BOTH:
                pass_on((y, z, 0), SIB)
        conv1d(0, first0)
        second0 = conv2(0, {5: four, 16: two_off})
        ready(1)
        arrange(1)
        first1 = conv1(1)
        pooled0 = conv2d(0, second0)
        margins(0, pooled0)
        conv1d(1, first1)
        second1 = conv2(1, {15: three_off})
        ready(2)
        arrange(2)
        first2 = conv1(2)
        pooled1 = conv2d(1, second1)
        margins(1, pooled1)
        ready(3)
        arrange(3)
        first3 = conv1(3)
        conv1d(2, first2)
        second2 = conv2(2, part=slice(0, 3))
        conv1d(3, first3)
        second3 = conv2(3)

        def far():
            margins(3, conv2d(3, second3))
            tell(3)

        conv2(2, {3: far}, second2, slice(3, None))
        margins(2, conv2d(2, second2))
        for g in (2, 1, 0):
            tell(g)

        assert len(sent) == SENDS
        pltpu.make_async_copy(gathered.at[pl.ds(0, SENDS)], gathered.at[pl.ds(0, SENDS)], fsend).wait()
        pltpu.make_async_copy(msg.at[pl.ds(1, n - 1)], msg.at[pl.ds(1, n - 1)], msend).wait()
        pltpu.make_async_copy(got.at[pl.ds(1, n - 1)], got.at[pl.ds(1, n - 1)], mrecv).wait()

    def rings(count, t):
        return tuple(
            tuple(tuple(pltpu.ACC(q)((t, TILE), jnp.float32) for _ in range(spots)) for q in range(2))
            for _ in range(count)
        )

    pl.run_scoped(body, rings(4, 16))


def finish(got, data_ref, mean_ref, norm_ref):
    n = got.shape[0]
    half = LANES // 2
    lane = lax.broadcasted_iota(jnp.int32, (n, LANES), 1)
    both = got[...]
    swapped = pltpu.roll(both, half, 1)
    margin = jnp.where(lane < half, both, swapped)
    identity = jnp.where(lane < half, swapped, both)
    mean = jnp.sum(margin, axis=0, keepdims=True) / n
    centred = margin - mean
    norm_ = jnp.sqrt(1.0 + jnp.sum(centred * centred, axis=0, keepdims=True) / n)
    scaled = centred / norm_
    for start in range(0, SUBSETS, LANES):
        here = identity == (lane + start).astype(jnp.float32)
        data_ref[:, start : start + LANES] = jnp.sum(jnp.where(here, scaled, 0.0), axis=0, keepdims=True)
    mean_ref[...] = mean[0, :1]
    norm_ref[...] = norm_[0, :1]


def shards(n, features, labels, subset_ids, conv1_weight, conv2_weight, head_weight):
    width, chans = features.shape[1], features.shape[3]
    offsets = conv1_weight.shape[1]
    spots = width * width
    assert features.shape[0] == 1 and conv1_weight.shape[0] == 1 and n == NY * NZ * 2
    head = jnp.transpose(head_weight, (2, 0, 1))
    anywhere = pl.BlockSpec(memory_space=pl.ANY)
    hbm = pl.BlockSpec(memory_space=pltpu.HBM)
    vmem = pl.BlockSpec(memory_space=pltpu.VMEM)
    got = pl.pallas_call(
        functools.partial(kernel, n),
        out_shape=pltpu.VMEM((n, LANES), jnp.float32),
        in_specs=[anywhere, hbm, hbm, anywhere, anywhere, anywhere],
        out_specs=vmem,
        scratch_shapes=[
            pltpu.VMEM((n, width, width, chans), features.dtype),
            pltpu.SMEM(labels.shape, labels.dtype),
            pltpu.SMEM(subset_ids.shape, subset_ids.dtype),
            pltpu.VMEM(conv1_weight.shape[1:], conv1_weight.dtype),
            pltpu.VMEM(conv2_weight.shape[1:], conv2_weight.dtype),
            pltpu.VMEM(head.shape, head.dtype),
            pltpu.VMEM((chans // LANES, n * spots, LANES), jnp.float32),
            pltpu.VMEM((n * spots, chans), jnp.float32),
            pltpu.VMEM((n, LANES), jnp.float32),
            pltpu.SemaphoreType.REGULAR((2,)),
            pltpu.SemaphoreType.DMA((2,)),
            pltpu.SemaphoreType.DMA,
            pltpu.SemaphoreType.DMA,
            pltpu.SemaphoreType.DMA,
            pltpu.SemaphoreType.DMA,
            pltpu.SemaphoreType.DMA,
            pltpu.SemaphoreType.DMA((n,)),
            pltpu.SemaphoreType.DMA((len(CHUNKS),)),
            pltpu.SemaphoreType.DMA,
            pltpu.SemaphoreType.DMA,
        ],
        compiler_params=pltpu.CompilerParams(
            collective_id=0, has_side_effects=True, vmem_limit_bytes=60 * 1024 * 1024
        ),
    )(features, labels, subset_ids, conv1_weight, conv2_weight, head)
    return pl.pallas_call(
        finish,
        out_shape=(
            jax.ShapeDtypeStruct((1, SUBSETS), jnp.float32),
            jax.ShapeDtypeStruct((1,), jnp.float32),
            jax.ShapeDtypeStruct((1,), jnp.float32),
        ),
        in_specs=[vmem],
        out_specs=(vmem, vmem, vmem),
    )(pltpu.with_memory_space_constraint(got, pltpu.VMEM))


def solution(mesh):
    in_specs = (
        P(("dp", "mp"), None, None, None),
        P("dp"),
        P("mp"),
        P("mp", None, None, None),
        P("mp", None, None, None),
        P("mp", None, None),
    )
    out_specs = (P(("dp", "mp"), None), P(("dp", "mp")), P(("dp", "mp")))
    return jax.shard_map(
        functools.partial(shards, mesh.shape["mp"]),
        mesh=mesh, in_specs=in_specs, out_specs=out_specs, check_vma=False,
    )
```

```python
import functools

import jax
import jax.numpy as jnp
from jax import lax
from jax.experimental import pallas as pl
from jax.experimental.pallas import tpu as pltpu
from jax.sharding import PartitionSpec as P

SUBSETS = 256
LANES = 128
TILE = 256
MESH = pl.DeviceIdType.MESH
NY, NZ = 4, 8
BOTH = (1, -1)

CHUNKS = [
    [(y, z, c) for c in (0, 1) for y, z in ((0, 0), (0, 1), (0, -1), (1, 0), (-1, 0), (0, 2), (0, -2), (2, 0))],
    [(y, z, 0) for y in BOTH for z in BOTH]
    + [(2, 1, 0), (2, -1, 0)]
    + [(y, 2 * z, 0) for y in BOTH for z in BOTH]
    + [(0, 3, 0), (0, -3, 0)]
    + [(y, z, 1) for y in BOTH for z in BOTH],
    [(2, 2, 0), (2, -2, 0), (0, 4, 0), (1, 3, 0), (-1, 3, 0), (0, 3, 1), (0, -3, 1), (2, 1, 1), (2, -1, 1)]
    + [(y, 2 * z, 1) for y in BOTH for z in BOTH]
    + [(2, 2, 1), (2, -2, 1), (0, 4, 1)],
    [(y, z, 0) for y, z in ((1, -3), (-1, -3), (2, 3), (2, -3), (1, 4), (-1, 4), (2, 4))]
    + [(y, z, 1) for y, z in ((1, -3), (-1, -3), (2, 3), (2, -3), (1, 4), (-1, 4), (2, 4), (1, 3), (-1, 3))],
]
STARTS = [sum(map(len, CHUNKS[:g])) for g in range(len(CHUNKS))]


def norm(r):
    dy, dz, dc = r
    dy, dz = dy % NY, dz % NZ
    return (dy - NY if dy > NY // 2 else dy, dz - NZ if dz > NZ // 2 else dz, dc % 2)


REL = sum(CHUNKS, [])
SLOT = {norm(r): i for i, r in enumerate(REL)}
CHUNK_OF = {norm(r): g for g, chunk in enumerate(CHUNKS) for r in chunk}
assert len(SLOT) == len(REL) == NY * NZ * 2


def minus(r, d):
    return norm((r[0] - d[0], r[1] - d[1], (r[2] + d[2]) % 2))


SIB, UP, DOWN, FAR = (0, 0, 1), (1, 0, 0), (-1, 0, 0), (2, 0, 0)
COLUMN = [FAR, UP, DOWN]
NEXT = [SIB, (0, 1, 0), (0, -1, 0), UP, DOWN, (0, 2, 0), (0, -2, 0), FAR]
SENDS = 63


def kernel(
    n, feat_ref, labels_ref, ids_ref, w1_ref, w2_ref, head_ref,
    got,
    gathered, labels, ids, w1, w2, head, grids, hids, msg,
    mid, small_sem, own_sem, w1_sem, w2_sem, head_sem, fsend, frecv, grecv, msend, mrecv,
):
    me = lax.axis_index("mp")
    my = lax.div(me, 2 * NZ)
    mz = lax.rem(lax.div(me, 2), NZ)
    mc = lax.rem(me, 2)
    width = feat_ref.shape[1]
    chans = feat_ref.shape[3]
    spots = width * width
    offsets = w1_ref.shape[1]
    classes = head_ref.shape[0]
    halves = chans // TILE

    def at(r):
        y = lax.rem(my + (r[0] % NY), NY)
        z = lax.rem(mz + (r[1] % NZ), NZ)
        c = mc if r[2] == 0 else 1 - mc
        return (y * NZ + z) * 2 + c

    own = pltpu.make_async_copy(feat_ref.at[0], gathered.at[0], own_sem)
    own.start()
    barrier = pltpu.get_barrier_semaphore()
    for r in NEXT:
        pl.semaphore_signal(barrier, inc=1, device_id={"mp": at(r)}, device_id_type=MESH)
    small_copies = [
        pltpu.make_async_copy(labels_ref, labels, small_sem.at[0]),
        pltpu.make_async_copy(ids_ref, ids, small_sem.at[1]),
    ]
    for copy in small_copies:
        copy.start()
    for o in range(offsets):
        pltpu.make_async_copy(w1_ref.at[0, o], w1.at[o], w1_sem).start()
    for o in range(offsets):
        pltpu.make_async_copy(w2_ref.at[0, o], w2.at[o], w2_sem).start()
    head_copy = pltpu.make_async_copy(head_ref, head, head_sem)
    head_copy.start()

    sent = []

    def send(r, d):
        s = SLOT[norm(r)]
        source = minus(r, d)
        there = SLOT[source]
        pltpu.make_async_remote_copy(
            src_ref=gathered.at[s], dst_ref=gathered.at[there],
            send_sem=fsend, recv_sem=grecv.at[CHUNK_OF[source]] if source[2] else frecv.at[there],
            device_id={"mp": at(d)}, device_id_type=MESH,
        ).start()
        sent.append(d)

    here = {(0, 0, 0)}

    def arrive(r):
        r = norm(r)
        if r in here:
            return
        here.add(r)
        s = SLOT[r]
        pltpu.make_async_copy(gathered.at[s], gathered.at[s], frecv.at[s]).wait()

    def pass_on(r, *where):
        arrive(r)
        for d in where:
            send(r, d)

    def ready(g):
        others = [r for r in CHUNKS[g] if r[2]]
        for r in CHUNKS[g]:
            if not r[2]:
                arrive(r)
        block = gathered.at[pl.ds(SLOT[norm(others[0])], len(others))]
        pltpu.make_async_copy(block, block, grecv.at[g]).wait()

    def body(rings):
        turns = []

        def take(t):
            turns.append(t)
            return rings[(len(turns) - 1) % len(rings)]

        def multiply(ring, lhs, tiles, between={}):
            for i, (rhs, pairs, depth) in enumerate(tiles):
                reg = i % 2
                for q in range(2):
                    pltpu.matmul_push_rhs(rhs(q), staging_register=reg, mxu_index=q)
                for j, (p, s) in enumerate(pairs):
                    x = lhs(s, depth)
                    for q in range(2):
                        pltpu.matmul_acc_lhs(ring[q][p], x, load_staged_rhs=reg if j == 0 else None)
                if i in between:
                    between[i]()

        def conv_tiles(kernel_ref):
            tiles = []
            for o in range(offsets):
                dy, dx = o // 3 - 1, o % 3 - 1
                pairs = [
                    (y * width + x, (y + dy) * width + x + dx)
                    for y in range(width)
                    for x in range(width)
                    if 0 <= y + dy < width and 0 <= x + dx < width
                ]
                for k in range(halves):
                    tiles.append((
                        lambda q, o=o, k=k: kernel_ref[o, k * TILE : (k + 1) * TILE, q * TILE : (q + 1) * TILE],
                        pairs, k,
                    ))
            return tiles

        def drain(ring):
            for p in range(spots):
                for q in range(2):
                    yield p, q, pltpu.matmul_pop(ring[q][p])

        def place(g, p, k):
            t = len(CHUNKS[g])
            first = STARTS[g] * spots + p * t
            return (slice(first, first + t), slice(k * TILE, (k + 1) * TILE))

        def arrange(g, span=(16,)):
            t = len(CHUNKS[g])
            for i in range(*span):
                for y in range(width):
                    first = STARTS[g] * spots + y * width * t + i
                    line = gathered[STARTS[g] + i, y].astype(jnp.float32)
                    for c in range(chans // LANES):
                        grids[c, pl.ds(first, width, stride=t), :] = line[:, c * LANES : (c + 1) * LANES]

        def grid(g, p, k):
            rows = place(g, p, k)[0]
            return jnp.concatenate([grids[c, rows, :] for c in range(k * TILE // LANES, (k + 1) * TILE // LANES)], 1)

        def conv1(g, between={}):
            ring = take(len(CHUNKS[g]))
            multiply(ring, lambda s, k: grid(g, s, k), conv_tiles(w1), between)
            return ring

        def conv1d(g, ring):
            for p, q, value in drain(ring):
                hids[place(g, p, q)] = jnp.maximum(value, 0.0)

        def conv2(g, between={}, ring=None, part=slice(None)):
            ring = ring or take(len(CHUNKS[g]))
            multiply(ring, lambda s, k: hids[place(g, s, k)], conv_tiles(w2)[part], between)
            return ring

        def conv2d(g, ring):
            pooled = [None] * 2
            for p, q, value in drain(ring):
                block = grid(g, p, q) + jnp.maximum(value, 0.0)
                pooled[q] = block if p == 0 else jnp.maximum(pooled[q], block)
            return pooled

        def margins(g, pooled):
            t = len(CHUNKS[g])
            sub = lax.broadcasted_iota(jnp.int32, (t, 1), 0)
            lane = lax.broadcasted_iota(jnp.int32, (t, LANES), 1)
            label = jnp.zeros((t, 1), jnp.int32)
            for i, r in enumerate(CHUNKS[g]):
                label = jnp.where(sub == i, labels[at(r)], label)
            correct = jnp.zeros((t, 1), jnp.float32)
            rival = jnp.full((t, 1), -1e30, jnp.float32)
            for k in range(classes):
                logit = jnp.sum(
                    pooled[0] * head[k, :, :TILE] + pooled[1] * head[k, :, TILE:], axis=1, keepdims=True
                )
                correct = jnp.where(label == k, logit, correct)
                rival = jnp.where(label == k, rival, jnp.maximum(rival, logit))
            identity = ids[0].astype(jnp.float32)
            first = STARTS[g]
            msg[first : first + t, :] = jnp.where(lane < LANES // 2, correct - rival, identity)

        def tell(g):
            first = STARTS[g]
            hops = [abs(r[0]) + abs(r[1]) for r in CHUNKS[g]]
            for i in sorted(range(len(hops)), key=lambda i: -hops[i]):
                r = CHUNKS[g][i]
                s = first + i
                if r == (0, 0, 0):
                    got[0:1, :] = msg[0:1, :]
                    continue
                there = SLOT[minus((0, 0, 0), r)]
                pltpu.make_async_remote_copy(
                    src_ref=msg.at[pl.ds(s, 1)], dst_ref=got.at[pl.ds(there, 1)],
                    send_sem=msend, recv_sem=mrecv,
                    device_id={"mp": at(r)}, device_id_type=MESH,
                ).start()

        for ring in rings:
            for q in range(2):
                for p in range(spots):
                    pltpu.matmul_pop(ring[q][p])
        pl.semaphore_wait(barrier, len(NEXT))
        for i, z in enumerate((2, -2)):
            pl.semaphore_signal(mid.at[i], inc=1, device_id={"mp": at((0, z, 0))}, device_id_type=MESH)
        own.wait()
        for d in NEXT:
            send((0, 0, 0), d)
        for i in range(2):
            pl.semaphore_wait(mid.at[i], 1)
        for z in (3, -3, 4):
            send((0, 0, 0), (0, z, 0))
        for z in BOTH:
            pass_on((0, z, 0), SIB, *COLUMN)
        for y in BOTH:
            pass_on((y, 0, 0), SIB)
        for z in BOTH:
            pass_on((0, 2 * z, 0), SIB, *COLUMN)
        pass_on((2, 0, 0), SIB)
        for copy in small_copies:
            copy.wait()
        pltpu.make_async_copy(w1, w1, w1_sem).wait()
        pltpu.make_async_copy(w2, w2, w2_sem).wait()
        head_copy.wait()
        arrange(0, (0, 8))
        ready(0)
        arrange(0, (8, 16))

        def four():
            for z in BOTH:
                pass_on((2, z, 0), SIB)
            pass_on((0, 4, 0), *COLUMN, *[(y, 0, 1) for y, _, _ in COLUMN], SIB)

        def two_off():
            for y in BOTH:
                for z in BOTH:
                    pass_on((y, 2 * z, 0), SIB)
            for z in BOTH:
                pass_on((2, 2 * z, 0), SIB)

        def three_off():
            for y in BOTH:
                for z in BOTH:
                    pass_on((y, 3 * z, 0), SIB)
            for z in BOTH:
                pass_on((2, 3 * z, 0), SIB)

        first0 = conv1(0)
        for y in BOTH:
            for z in BOTH:
                pass_on((y, z, 0), SIB)
        for z in BOTH:
            pass_on((0, 3 * z, 0), *COLUMN, SIB)
        conv1d(0, first0)
        second0 = conv2(0, {4: four})
        ready(1)
        arrange(1)
        first1 = conv1(1, {1: two_off})
        pooled0 = conv2d(0, second0)
        margins(0, pooled0)
        conv1d(1, first1)
        second1 = conv2(1, {14: three_off})
        ready(2)
        arrange(2)
        first2 = conv1(2)
        pooled1 = conv2d(1, second1)
        margins(1, pooled1)
        ready(3)
        arrange(3)
        first3 = conv1(3)
        conv1d(2, first2)
        second2 = conv2(2, part=slice(0, 3))
        conv1d(3, first3)
        second3 = conv2(3)

        def far():
            margins(3, conv2d(3, second3))
            tell(3)

        conv2(2, {3: far}, second2, slice(3, None))
        margins(2, conv2d(2, second2))
        for g in (2, 1, 0):
            tell(g)

        assert len(sent) == SENDS
        pltpu.make_async_copy(gathered.at[pl.ds(0, SENDS)], gathered.at[pl.ds(0, SENDS)], fsend).wait()
        pltpu.make_async_copy(msg.at[pl.ds(1, n - 1)], msg.at[pl.ds(1, n - 1)], msend).wait()
        pltpu.make_async_copy(got.at[pl.ds(1, n - 1)], got.at[pl.ds(1, n - 1)], mrecv).wait()

    def rings(count, t):
        return tuple(
            tuple(tuple(pltpu.ACC(q)((t, TILE), jnp.float32) for _ in range(spots)) for q in range(2))
            for _ in range(count)
        )

    pl.run_scoped(body, rings(4, 16))


def finish(got, data_ref, mean_ref, norm_ref):
    n = got.shape[0]
    half = LANES // 2
    lane = lax.broadcasted_iota(jnp.int32, (n, LANES), 1)
    both = got[...]
    swapped = pltpu.roll(both, half, 1)
    margin = jnp.where(lane < half, both, swapped)
    identity = jnp.where(lane < half, swapped, both)
    mean = jnp.sum(margin, axis=0, keepdims=True) / n
    centred = margin - mean
    norm_ = jnp.sqrt(1.0 + jnp.sum(centred * centred, axis=0, keepdims=True) / n)
    scaled = centred / norm_
    for start in range(0, SUBSETS, LANES):
        here = identity == (lane + start).astype(jnp.float32)
        data_ref[:, start : start + LANES] = jnp.sum(jnp.where(here, scaled, 0.0), axis=0, keepdims=True)
    mean_ref[...] = mean[0, :1]
    norm_ref[...] = norm_[0, :1]


def shards(n, features, labels, subset_ids, conv1_weight, conv2_weight, head_weight):
    width, chans = features.shape[1], features.shape[3]
    offsets = conv1_weight.shape[1]
    spots = width * width
    assert features.shape[0] == 1 and conv1_weight.shape[0] == 1 and n == NY * NZ * 2
    head = jnp.transpose(head_weight, (2, 0, 1))
    anywhere = pl.BlockSpec(memory_space=pl.ANY)
    hbm = pl.BlockSpec(memory_space=pltpu.HBM)
    vmem = pl.BlockSpec(memory_space=pltpu.VMEM)
    got = pl.pallas_call(
        functools.partial(kernel, n),
        out_shape=pltpu.VMEM((n, LANES), jnp.float32),
        in_specs=[anywhere, hbm, hbm, anywhere, anywhere, anywhere],
        out_specs=vmem,
        scratch_shapes=[
            pltpu.VMEM((n, width, width, chans), features.dtype),
            pltpu.SMEM(labels.shape, labels.dtype),
            pltpu.SMEM(subset_ids.shape, subset_ids.dtype),
            pltpu.VMEM(conv1_weight.shape[1:], conv1_weight.dtype),
            pltpu.VMEM(conv2_weight.shape[1:], conv2_weight.dtype),
            pltpu.VMEM(head.shape, head.dtype),
            pltpu.VMEM((chans // LANES, n * spots, LANES), jnp.float32),
            pltpu.VMEM((n * spots, chans), jnp.float32),
            pltpu.VMEM((n, LANES), jnp.float32),
            pltpu.SemaphoreType.REGULAR((2,)),
            pltpu.SemaphoreType.DMA((2,)),
            pltpu.SemaphoreType.DMA,
            pltpu.SemaphoreType.DMA,
            pltpu.SemaphoreType.DMA,
            pltpu.SemaphoreType.DMA,
            pltpu.SemaphoreType.DMA,
            pltpu.SemaphoreType.DMA((n,)),
            pltpu.SemaphoreType.DMA((len(CHUNKS),)),
            pltpu.SemaphoreType.DMA,
            pltpu.SemaphoreType.DMA,
        ],
        compiler_params=pltpu.CompilerParams(
            collective_id=0, has_side_effects=True, vmem_limit_bytes=60 * 1024 * 1024
        ),
    )(features, labels, subset_ids, conv1_weight, conv2_weight, head)
    return pl.pallas_call(
        finish,
        out_shape=(
            jax.ShapeDtypeStruct((1, SUBSETS), jnp.float32),
            jax.ShapeDtypeStruct((1,), jnp.float32),
            jax.ShapeDtypeStruct((1,), jnp.float32),
        ),
        in_specs=[vmem],
        out_specs=(vmem, vmem, vmem),
    )(pltpu.with_memory_space_constraint(got, pltpu.VMEM))


def solution(mesh):
    in_specs = (
        P(("dp", "mp"), None, None, None),
        P("dp"),
        P("mp"),
        P("mp", None, None, None),
        P("mp", None, None, None),
        P("mp", None, None),
    )
    out_specs = (P(("dp", "mp"), None), P(("dp", "mp")), P(("dp", "mp")))
    return jax.shard_map(
        functools.partial(shards, mesh.shape["mp"]),
        mesh=mesh, in_specs=in_specs, out_specs=out_specs, check_vma=False,
    )
```
